8 devices in a mesh: rep: 2 (over z, y), data: 4 (over x, core).
Axes of the slice: x: 2, y: 2, z: 1, core: 2. Of those that a mesh axis runs over, the one named last changes fastest.
Arguments:
- W_in: float32 [12288, 768], P('rep'), parts along dimension 0
- W1: float32 [6, 768, 3072], P('rep'), parts along dimension 0
- W2: float32 [6, 3072, 768], P('rep'), parts along dimension 0
- m_in: float32 [12288, 768], P('rep'), parts along dimension 0
- v_in: float32 [12288, 768], P('rep'), parts along dimension 0
- m1: float32 [6, 768, 3072], P('rep'), parts along dimension 0
- v1: float32 [6, 768, 3072], P('rep'), parts along dimension 0
- m2: float32 [6, 3072, 768], P('rep'), parts along dimension 0
- v2: float32 [6, 3072, 768], P('rep'), parts along dimension 0
- X0: bfloat16 [16384, 6144], P(('rep', 'data')), parts along dimension 0
- Y0: bfloat16 [16384, 768], P(('rep', 'data')), parts along dimension 0
- X1: bfloat16 [16384, 6144], P(('rep', 'data')), parts along dimension 0
- Y1: bfloat16 [16384, 768], P(('rep', 'data')), parts along dimension 0
Outputs:
- output 1: float32 [12288, 768], P('rep'), parts along dimension 0
- output 2: float32 [6, 768, 3072], P('rep'), parts along dimension 0
- output 3: float32 [6, 3072, 768], P('rep'), parts along dimension 0
- output 4: float32 [12288, 768], P('rep'), parts along dimension 0
- output 5: float32 [12288, 768], P('rep'), parts along dimension 0
- output 6: float32 [6, 768, 3072], P('rep'), parts along dimension 0
- output 7: float32 [6, 768, 3072], P('rep'), parts along dimension 0
- output 8: float32 [6, 3072, 768], P('rep'), parts along dimension 0
- output 9: float32 [6, 3072, 768], P('rep'), parts along dimension 0
- output 10: float32 [16384], P(('rep', 'data')), parts along dimension 0
- output 11: float32 [16384, 768], P(('rep', 'data')), parts along dimension 0
There are 2 independent parts. The reference program is written for one: setup_inputs(seed, part) draws one part's arguments, and reference() takes and returns one part's arrays. A program takes and returns all parts, laid end to end along the dimension named above; each array names one.
All inputs are finite; a program needn't handle non-finite values.
Results may differ from the reference program's by a relative error of at most 0.0144442.
Values are sent between devices in bfloat16 or wider.
A program may use at most 2 GiB of HBM per device.

```python
import jax
import jax.numpy as jnp
from jax import lax

TOK = 2048
DATA = 4
L = 3
D = 768
F = 3072
E = 6144

N = TOK * DATA
BETA1 = 0.9
BETA2 = 0.999
BC1 = 1.0 / (1.0 - BETA1 ** 10)
BC2 = 1.0 / (1.0 - BETA2 ** 10)
EPS = 1e-12
WD = 0.01
ETA = 0.05
R2 = 0.7071067811865476
R2PI = 0.3989422804014327


def gelu_grad(a):
    return 0.5 * (1.0 + lax.erf(a * R2)) + a * jnp.exp(-0.5 * a * a) * R2PI


def loss_f32(wi, w1, w2, x, y):
    def layer(h, w):
        return h + jnp.dot(jax.nn.gelu(jnp.dot(h, w[0]), approximate=False), w[1]), None
    h, _ = lax.scan(layer, jnp.dot(x, wi), (w1, w2))
    return jnp.sum((h - y) ** 2) / (2.0 * N * D)


def tokens(key, width):
    k1, k2, k3 = jax.random.split(key, 3)
    mu = jax.random.normal(k1, (DATA, 1, width), jnp.float32)
    sc = jax.random.uniform(k2, (DATA, 1, 1), jnp.float32, 0.5, 1.5)
    z = jax.random.normal(k3, (DATA, TOK, width), jnp.float32)
    return (z * sc + mu).reshape(N, width).astype(jnp.bfloat16)


def rms(g):
    return jnp.sqrt(jnp.mean(g * g, axis=(-2, -1), keepdims=True))


def moments(key, s, shape):
    ka, kb = jax.random.split(key)
    m = 0.1 * s * jax.random.normal(ka, shape, jnp.float32)
    v = 1e-3 * s * s * jax.random.uniform(kb, shape, jnp.float32, 0.5, 1.5)
    return m, v


def setup_inputs(seed: int = 0, part: int = 0) -> dict:
    ks = jax.random.split(jax.random.fold_in(jax.random.key(seed), part), 10)
    wi = jax.random.normal(ks[0], (E, D), jnp.float32) * E ** -0.5
    w1 = jax.random.normal(ks[1], (L, D, F), jnp.float32) * D ** -0.5
    w2 = jax.random.normal(ks[2], (L, F, D), jnp.float32) * (0.5 * F ** -0.5)
    x0 = tokens(ks[3], E)
    y0 = tokens(ks[4], D)
    x1 = tokens(ks[5], E)
    y1 = tokens(ks[6], D)
    gi, g1, g2 = jax.grad(loss_f32, argnums=(0, 1, 2))(wi, w1, w2, x0.astype(jnp.float32), y0.astype(jnp.float32))
    mi, vi = moments(ks[7], rms(gi), (E, D))
    m1, v1 = moments(ks[8], rms(g1), (L, D, F))
    m2, v2 = moments(ks[9], rms(g2), (L, F, D))
    return {'W_in': wi, 'W1': w1, 'W2': w2, 'm_in': mi, 'v_in': vi, 'm1': m1, 'v1': v1, 'm2': m2, 'v2': v2, 'X0': x0, 'Y0': y0, 'X1': x1, 'Y1': y1}


def forward_saved(wib, w1b, w2b, x):
    def layer(h, w):
        a = jnp.dot(h.astype(jnp.bfloat16), w[0], preferred_element_type=jnp.float32)
        s = jax.nn.gelu(a, approximate=False).astype(jnp.bfloat16)
        return h + jnp.dot(s, w[1], preferred_element_type=jnp.float32), (h, a)
    return lax.scan(layer, jnp.dot(x, wib, preferred_element_type=jnp.float32), (w1b, w2b))


def forward(wib, w1b, w2b, x):
    def layer(h, w):
        a = jnp.dot(h.astype(jnp.bfloat16), w[0], preferred_element_type=jnp.float32)
        s = jax.nn.gelu(a, approximate=False).astype(jnp.bfloat16)
        return h + jnp.dot(s, w[1], preferred_element_type=jnp.float32), None
    h, _ = lax.scan(layer, jnp.dot(x, wib, preferred_element_type=jnp.float32), (w1b, w2b))
    return h


def local_grads(wib, w1b, w2b, x, y):
    hl, (hs, acts) = forward_saved(wib, w1b, w2b, x)

    def back(g, inp):
        h, a, w1, w2 = inp
        gb = g.astype(jnp.bfloat16)
        s = jax.nn.gelu(a, approximate=False).astype(jnp.bfloat16)
        dw2 = jnp.dot(s.T, gb, preferred_element_type=jnp.float32).astype(jnp.bfloat16)
        e = (jnp.dot(gb, w2.T, preferred_element_type=jnp.float32) * gelu_grad(a)).astype(jnp.bfloat16)
        dw1 = jnp.dot(h.astype(jnp.bfloat16).T, e, preferred_element_type=jnp.float32).astype(jnp.bfloat16)
        return g + jnp.dot(e, w1.T, preferred_element_type=jnp.float32), (dw1, dw2)

    g_last = (hl - y.astype(jnp.float32)) * (1.0 / (N * D))
    g0, (dw1, dw2) = lax.scan(back, g_last, (hs, acts, w1b, w2b), reverse=True)
    dwi = jnp.dot(x.T, g0.astype(jnp.bfloat16), preferred_element_type=jnp.float32).astype(jnp.bfloat16)
    return dwi, dw1, dw2


def lamb(w, g, m, v):
    m2 = BETA1 * m + (1.0 - BETA1) * g
    v2 = BETA2 * v + (1.0 - BETA2) * g * g
    u = BC1 * m2 / (jnp.sqrt(BC2 * v2) + EPS) + WD * w
    r = jnp.sqrt(jnp.sum(w * w, axis=(-2, -1), keepdims=True)) / jnp.sqrt(jnp.sum(u * u, axis=(-2, -1), keepdims=True))
    return w - ETA * r * u, m2, v2


def reference(W_in, W1, W2, m_in, v_in, m1, v1, m2, v2, X0, Y0, X1, Y1):
    wib = W_in.astype(jnp.bfloat16)
    w1b = W1.astype(jnp.bfloat16)
    w2b = W2.astype(jnp.bfloat16)

    def acc(c, xy):
        gi, g1, g2 = local_grads(wib, w1b, w2b, xy[0], xy[1])
        return (c[0] + gi.astype(jnp.float32), c[1] + g1.astype(jnp.float32), c[2] + g2.astype(jnp.float32)), None

    zero = (jnp.zeros((E, D), jnp.float32), jnp.zeros((L, D, F), jnp.float32), jnp.zeros((L, F, D), jnp.float32))
    (gi, g1, g2), _ = lax.scan(acc, zero, (X0.reshape(DATA, TOK, E), Y0.reshape(DATA, TOK, D)))
    wi_n, mi_n, vi_n = lamb(W_in, gi.astype(jnp.bfloat16).astype(jnp.float32), m_in, v_in)
    w1_n, m1_n, v1_n = lamb(W1, g1.astype(jnp.bfloat16).astype(jnp.float32), m1, v1)
    w2_n, m2_n, v2_n = lamb(W2, g2.astype(jnp.bfloat16).astype(jnp.float32), m2, v2)
    nwi = wi_n.astype(jnp.bfloat16)
    nw1 = w1_n.astype(jnp.bfloat16)
    nw2 = w2_n.astype(jnp.bfloat16)
    h = lax.map(lambda xb: forward(nwi, nw1, nw2, xb), X1.reshape(DATA, TOK, E)).reshape(N, D)
    loss = jnp.sum((h - Y1.astype(jnp.float32)) ** 2, axis=-1) / (2.0 * D)
    return (wi_n, w1_n, w2_n, mi_n, vi_n, m1_n, v1_n, m2_n, v2_n, loss, h)
```

```python
import functools

import jax
import jax.numpy as jnp
from jax import lax
from jax.experimental import pallas as pl
from jax.experimental.pallas import tpu as pltpu
from jax.sharding import PartitionSpec as P

BETA1 = 0.9
BETA2 = 0.999
BC1 = 1.0 / (1.0 - BETA1 ** 10)
BC2 = 1.0 / (1.0 - BETA2 ** 10)
EPS = 1e-12
WD = 0.01
ETA = 0.05
R2 = 0.7071067811865476
R2PI = 0.3989422804014327
BF = jnp.bfloat16
F32 = jnp.float32
VMEM = 67043328
ANY = pl.BlockSpec(memory_space=pl.ANY)

D2D = [(0, 1), (1, 0), (2, 3), (3, 2)]
CROSS = [(0, 2), (2, 0), (1, 3), (3, 1)]
DIAG = [(0, 3), (3, 0), (1, 2), (2, 1)]


def dot(a, b):
    return jnp.dot(a, b, preferred_element_type=F32)


def dot_nt(a, b):
    return lax.dot_general(a, b, (((1,), (1,)), ((), ())), preferred_element_type=F32)


def dot_tn(a, b):
    return lax.dot_general(a, b, (((0,), (0,)), ((), ())), preferred_element_type=F32)


def gelu(a):
    return (0.5 * a) * (1.0 + lax.erf(a * R2))


def gelu_grad(a):
    return 0.5 * (1.0 + lax.erf(a * R2)) + a * jnp.exp(-0.5 * a * a) * R2PI


def params(*sem):
    return pltpu.CompilerParams(vmem_limit_bytes=VMEM, dimension_semantics=sem)


def cost(flops, nbytes):
    return pl.CostEstimate(flops=int(flops), bytes_accessed=int(nbytes), transcendentals=0)


def in_kernel(x_ref, w_ref, o_ref):
    @pl.when(pl.program_id(0) == 0)
    def _():
        o_ref[...] = jnp.zeros_like(o_ref)

    o_ref[...] += dot(x_ref[...], w_ref[...].astype(BF))


def in_matmul(x, w, kb=768):
    t, e = x.shape
    d = w.shape[1]
    return pl.pallas_call(
        in_kernel,
        grid=(e // kb,),
        in_specs=[pl.BlockSpec((t, kb), lambda k: (0, k)), pl.BlockSpec((kb, d), lambda k: (k, 0))],
        out_specs=pl.BlockSpec((t, d), lambda k: (0, 0)),
        out_shape=jax.ShapeDtypeStruct((t, d), F32),
        compiler_params=params("arbitrary"),
        cost_estimate=cost(2 * t * e * d, 2 * t * e + w.nbytes + 4 * t * d),
        name="in_matmul",
    )(x, w)


def chain_kernel(scale, dev, nm, c_ref, h_ref, y_ref, w1_hbm, w2_hbm, *rest):
    hb_o, s_o, gb_o, e_o, g0_o, w1, w2, a_s, s_s, h_s, sem = rest[4 * (dev > 0):]
    t = pl.program_id(0)
    c = c_ref[0]
    nl, _, f = w1.shape
    half = f // 2
    fc = half // nm

    def copies(l):
        out = []
        for k in range(2):
            src = pl.multiple_of(lax.rem(c + k, 2) * half, half)
            out.append(pltpu.make_async_copy(w1_hbm.at[l, :, pl.ds(src, half)], w1.at[l, :, pl.ds(k * half, half)],
                                             sem.at[l, k]))
            out.append(pltpu.make_async_copy(w2_hbm.at[l, pl.ds(src, half), :], w2.at[l, pl.ds(k * half, half), :],
                                             sem.at[l, k + 2]))
        return out

    @pl.when(t == 0)
    def _():
        for l in range(nl):
            for cp in copies(l):
                cp.start()

    h_s[...] = h_ref[...]

    def piece(o, l, j):
        return o.at[0, l, :, j * fc:(j + 1) * fc] if j < nm else s_s.at[:, (j - nm) * fc:(j - nm + 1) * fc]

    def fwd(l, carry):
        @pl.when(t == 0)
        def _():
            for cp in copies(l):
                cp.wait()

        hb_o[0, l] = h_s[...].astype(BF)

        def up(j):
            a_s[l, :, j * fc:(j + 1) * fc] = dot(hb_o[0, l], w1[l, :, j * fc:(j + 1) * fc])

        up(0)
        for j in range(2 * nm):
            if j + 1 < 2 * nm:
                up(j + 1)
            piece(s_o, l, j)[...] = gelu(a_s[l, :, j * fc:(j + 1) * fc]).astype(BF)
            h_s[...] += dot(piece(s_o, l, j)[...], w2[l, j * fc:(j + 1) * fc, :])
        return carry

    def bwd(k, carry):
        l = nl - 1 - k
        gb_o[0, l] = h_s[...].astype(BF)

        def down(j):
            return dot_nt(gb_o[0, l], w2[l, j * fc:(j + 1) * fc, :])

        de = down(0)
        for j in range(2 * nm):
            nxt = down(j + 1) if j + 1 < 2 * nm else None
            piece(e_o, l, j)[...] = (de * gelu_grad(a_s[l, :, j * fc:(j + 1) * fc])).astype(BF)
            h_s[...] += dot_nt(piece(e_o, l, j)[...], w1[l, :, j * fc:(j + 1) * fc])
            de = nxt
        return carry

    lax.fori_loop(0, nl, fwd, 0)
    h_s[...] = (h_s[...] - y_ref[...].astype(F32)) * scale
    lax.fori_loop(0, nl, bwd, 0)
    g0_o[...] = h_s[...].astype(BF)


def chain(c, h, y, w1, w2, scale, prev=None, tm=256, nm=2):
    t, d = h.shape
    nl, _, f = w1.shape
    half = f // 2
    dev = 0 if prev is None else 1
    tok = pl.BlockSpec((tm, d), lambda i, c: (i, 0))

    def out(w):
        return pl.BlockSpec((1, nl, tm, w), lambda i, c: (dev, 0, i, 0))

    shapes = [jax.ShapeDtypeStruct((2, nl, t, w), BF) for w in (d, half, d, half)]
    return pl.pallas_call(
        functools.partial(chain_kernel, scale, dev, nm),
        grid_spec=pltpu.PrefetchScalarGridSpec(
            num_scalar_prefetch=1,
            grid=(t // tm,),
            in_specs=[tok, tok, ANY, ANY] + [ANY] * (4 * dev),
            out_specs=[out(d), out(half), out(d), out(half), tok],
            scratch_shapes=[
                pltpu.VMEM((nl, d, f), BF),
                pltpu.VMEM((nl, f, d), BF),
                pltpu.VMEM((nl, tm, f), F32),
                pltpu.VMEM((tm, half), BF),
                pltpu.VMEM((tm, d), F32),
                pltpu.SemaphoreType.DMA((nl, 4)),
            ],
        ),
        out_shape=shapes + [jax.ShapeDtypeStruct((t, d), BF)],
        input_output_aliases={5 + k: k for k in range(4 * dev)},
        compiler_params=params("arbitrary"),
        cost_estimate=cost(8 * nl * t * d * f, 4 * nl * d * f + 8 * t * d + 4 * nl * t * (d + half)),
        name="chain_%d" % dev,
    )(c, h, y, w1, w2, *(prev or ()))


def dw_kernel(i_ref, hb_ref, s_ref, gb_ref, e_ref, sp_o, sm_o, acc):
    job, dev, k = pl.program_id(0), pl.program_id(1), pl.program_id(2)
    nk = pl.num_programs(2)

    def product(a_ref, b_ref):
        acc[...] = jnp.where(k == 0, 0.0, acc[...]) + dot_tn(a_ref[0, 0], b_ref[0, 0])

    @pl.when(job % 2 == 0)
    def _():
        product(s_ref, gb_ref)

    @pl.when(job % 2 == 1)
    def _():
        product(hb_ref, e_ref)

    def add(o):
        r = acc[...].astype(BF).astype(F32)
        o[0] = jnp.where(dev == 0, 0.0, o[0]) + r

    @pl.when((k == nk - 1) & (job < 2))
    def _():
        add(sp_o)

    @pl.when((k == nk - 1) & (job >= 2))
    def _():
        add(sm_o)


def dw_half(core, acts, l, kb=1024):
    hb, s, gb, e = acts
    t, d = hb.shape[2:]
    q = s.shape[3] // 2

    def quarter(job, core):
        return jnp.where(job < 2, 1 - core, core)

    def feat(odd):
        def index(job, dev, k, c):
            mine = job % 2 == odd
            return (jnp.where(mine, dev, 0), l, jnp.where(mine, k, 0), quarter(job, c[0]))
        return index

    def full(odd):
        def index(job, dev, k, c):
            mine = job % 2 == odd
            return (jnp.where(mine, dev, 0), l, jnp.where(mine, k, 0), 0)
        return index

    blk = (1, 1, kb, q)
    return pl.pallas_call(
        dw_kernel,
        grid_spec=pltpu.PrefetchScalarGridSpec(
            num_scalar_prefetch=1,
            grid=(4, 2, t // kb),
            in_specs=[pl.BlockSpec((1, 1, kb, d), full(1)), pl.BlockSpec(blk, feat(0)),
                      pl.BlockSpec((1, 1, kb, d), full(0)), pl.BlockSpec(blk, feat(1))],
            out_specs=[pl.BlockSpec((1, d, d), lambda job, dev, k, c: (jnp.minimum(job, 1), 0, 0)),
                       pl.BlockSpec((1, d, d), lambda job, dev, k, c: (jnp.maximum(job - 2, 0), 0, 0))],
            scratch_shapes=[pltpu.VMEM((d, d), F32)],
        ),
        out_shape=[jax.ShapeDtypeStruct((2, d, d), F32)] * 2,
        compiler_params=params("arbitrary", "arbitrary", "arbitrary"),
        cost_estimate=cost(16 * t * d * d, 16 * t * d * 2 + 16 * d * d),
        name="dw_%d" % l,
    )(core, hb, s, gb, e)


def dwi_kernel(q_ref, x_ref, g_ref, o_ref):
    o_ref[...] = dot_tn(x_ref[...], g_ref[...]).astype(BF)


def dwi_quarter(q, x, g, mb=512):
    t, e = x.shape
    d = g.shape[1]
    n = e // 4 // mb
    return pl.pallas_call(
        dwi_kernel,
        grid_spec=pltpu.PrefetchScalarGridSpec(
            num_scalar_prefetch=1,
            grid=(n,),
            in_specs=[pl.BlockSpec((t, mb), lambda j, q: (0, q[0] * n + j)), pl.BlockSpec((t, d), lambda j, q: (0, 0))],
            out_specs=pl.BlockSpec((mb, d), lambda j, q: (j, 0)),
        ),
        out_shape=jax.ShapeDtypeStruct((e // 4, d), BF),
        compiler_params=params("arbitrary"),
        cost_estimate=cost(2 * t * e * d // 4, t * e // 2 + 2 * t * d),
        name="dwi",
    )(q, x, g)


def lamb_kernel(nb, gi, i_ref, *refs):
    w_ref, m_ref, v_ref, g0, g1, g2, g3 = refs[:7]
    wn_o, mn_o, vn_o, wb_o, w_s, u_s, sw, su, ratio = refs[-9:]
    p, k, j = pl.program_id(0), pl.program_id(1), pl.program_id(2)
    slot = k * nb + j
    shape = w_s.shape[1:]
    first = (k == 0) & (j == 0)

    @pl.when((p == 0) & first)
    def _():
        sw[...] = jnp.zeros_like(sw)
        su[...] = jnp.zeros_like(su)

    def sweep(g_ref):
        w = w_ref[...].reshape(shape)
        g = g_ref[...].reshape(shape).astype(F32)
        m2 = BETA1 * m_ref[...].reshape(shape) + (1.0 - BETA1) * g
        v2 = BETA2 * v_ref[...].reshape(shape) + (1.0 - BETA2) * g * g
        u = BC1 * m2 / (jnp.sqrt(BC2 * v2) + EPS) + WD * w
        mn_o[...] = m2.reshape(mn_o.shape)
        vn_o[...] = v2.reshape(vn_o.shape)
        w_s[slot] = w
        u_s[slot] = u
        sw[...] += jnp.sum((w * w).reshape(-1, 8, shape[1]), axis=0)
        su[...] += jnp.sum((u * u).reshape(-1, 8, shape[1]), axis=0)

    for kk, g_ref in enumerate((g0, g1, g2, g3)):
        @pl.when((p == 0) & (k == kk))
        def _(g_ref=g_ref):
            sweep(g_ref)

    @pl.when((p == 1) & first)
    def _():
        ratio[0] = ETA * (jnp.sqrt(jnp.sum(sw[...])) / jnp.sqrt(jnp.sum(su[...])))

    @pl.when(p == 1)
    def _():
        w = w_s[slot] - ratio[0] * u_s[slot]
        wn_o[...] = w.reshape(wn_o.shape)
        wb_o[...] = w.astype(BF)


def lamb(i, w, m, v, gs, gi, l, bufs, cols, rb):
    rows, width = w.shape[-2:]
    gr, gw = gs[0].shape[-2:]
    nb = gr // rb
    lead = () if l is None else (l,)
    one = () if l is None else (1,)

    def where(p, k, j, i):
        q = jnp.bitwise_xor(k, i[0])
        return (j, q) if cols else (q * nb + j, 0)

    def at_first(p, k, j, i):
        k, j = jnp.where(p == 0, k, 3), jnp.where(p == 0, j, nb - 1)
        return lead + where(p, k, j, i)

    def at_second(p, k, j, i):
        k, j = jnp.where(p == 1, k, 0), jnp.where(p == 1, j, 0)
        return lead + where(p, k, j, i)

    def at_second2(p, k, j, i):
        k, j = jnp.where(p == 1, k, 0), jnp.where(p == 1, j, 0)
        return where(p, k, j, i)

    def at_g(kk):
        def index(p, k, j, i):
            b = jnp.where((p == 1) | (k > kk), nb - 1, jnp.where(k < kk, 0, j))
            return (b, 0) if gi is None else (gi, b, 0)
        return index

    blk = one + (rb, gw)
    gblk = (rb, gw) if gi is None else (1, rb, gw)
    n = len(bufs)
    f32 = jax.ShapeDtypeStruct(w.shape, F32)
    return pl.pallas_call(
        functools.partial(lamb_kernel, nb, gi),
        grid_spec=pltpu.PrefetchScalarGridSpec(
            num_scalar_prefetch=1,
            grid=(2, 4, nb),
            in_specs=[pl.BlockSpec(blk, at_first)] * 3 + [pl.BlockSpec(gblk, at_g(kk)) for kk in range(4)] + [ANY] * n,
            out_specs=[pl.BlockSpec(blk, at_second), pl.BlockSpec(blk, at_first), pl.BlockSpec(blk, at_first),
                       pl.BlockSpec((rb, gw), at_second2)],
            scratch_shapes=[
                pltpu.VMEM((4 * nb, rb, gw), F32),
                pltpu.VMEM((4 * nb, rb, gw), F32),
                pltpu.VMEM((8, gw), F32),
                pltpu.VMEM((8, gw), F32),
                pltpu.SMEM((1,), F32),
            ],
        ),
        out_shape=[f32, f32, f32, jax.ShapeDtypeStruct((rows, width), BF)],
        input_output_aliases={8 + k: k for k in range(n)},
        compiler_params=params("arbitrary", "arbitrary", "arbitrary"),
        cost_estimate=cost(30 * rows * width * 30, 28 * rows * width),
        name="lamb",
    )(i, w, m, v, *gs, *bufs)


def fwd_kernel(nl, nj, h_ref, *refs):
    w1_hbm, w2_hbm = refs[:nl], refs[nl:2 * nl]
    o_ref, w1, w2, a_s, s_s, sem = refs[2 * nl:]
    t = pl.program_id(0)
    fc = w1.shape[2] // nj

    @pl.when(t == 0)
    def _():
        for l in range(nl):
            pltpu.make_async_copy(w1_hbm[l], w1.at[l], sem.at[l, 0]).start()
            pltpu.make_async_copy(w2_hbm[l], w2.at[l], sem.at[l, 1]).start()

    o_ref[...] = h_ref[...]

    def layer(l, carry):
        @pl.when(t == 0)
        def _():
            pltpu.make_async_copy(w1_hbm[0], w1.at[l], sem.at[l, 0]).wait()
            pltpu.make_async_copy(w2_hbm[0], w2.at[l], sem.at[l, 1]).wait()

        hb = o_ref[...].astype(BF)

        def up(j):
            a_s[:, j * fc:(j + 1) * fc] = dot(hb, w1[l, :, j * fc:(j + 1) * fc])

        up(0)
        for j in range(nj):
            if j + 1 < nj:
                up(j + 1)
            s_s[:, j * fc:(j + 1) * fc] = gelu(a_s[:, j * fc:(j + 1) * fc]).astype(BF)
            o_ref[...] += dot(s_s[:, j * fc:(j + 1) * fc], w2[l, j * fc:(j + 1) * fc, :])
        return carry

    lax.fori_loop(0, nl, layer, 0)


def forward(h, w1, w2, tm=256, nj=4):
    t, d = h.shape
    nl = len(w1)
    f = w1[0].shape[1]
    tok = pl.BlockSpec((tm, d), lambda i: (i, 0))
    return pl.pallas_call(
        functools.partial(fwd_kernel, nl, nj),
        grid=(t // tm,),
        in_specs=[tok] + [ANY] * (2 * nl),
        out_specs=tok,
        out_shape=jax.ShapeDtypeStruct((t, d), F32),
        scratch_shapes=[
            pltpu.VMEM((nl, d, f), BF),
            pltpu.VMEM((nl, f, d), BF),
            pltpu.VMEM((tm, f), F32),
            pltpu.VMEM((tm, f), BF),
            pltpu.SemaphoreType.DMA((nl, 2)),
        ],
        compiler_params=params("arbitrary"),
        cost_estimate=cost(4 * nl * t * d * f, 4 * nl * d * f + 8 * t * d),
        name="forward",
    )(h, *w1, *w2)


def solution(mesh):
    p = mesh.shape['data']

    def step(wi, w1, w2, mi, vi, m1, v1, m2, v2, x0, y0, x1, y1):
        nl, d, f = w1.shape
        scale = 1.0 / (x0.shape[0] * p * d)
        i = lax.axis_index('data').astype(jnp.int32)
        me = jnp.reshape(i, (1,))
        chip = me // 2
        core = me % 2

        def send(x, perm):
            return lax.ppermute(x, 'data', perm)

        def gather(g):
            far = send(g, CROSS)
            return g, send(g, D2D), far, send(far, D2D)

        w1b, w2b = w1.astype(BF), w2.astype(BF)
        y0o = send(y0, CROSS)
        h0 = in_matmul(x0, wi)
        h0o = send(h0, CROSS)
        *acts, g0 = chain(chip, h0, y0, w1b, w2b, scale)
        pieces = {k: dwi_quarter(jnp.bitwise_xor(me, k), x0, g0) for k in (2, 3, 1, 0)}
        got = [pieces[0], send(pieces[1], D2D), send(pieces[2], CROSS), send(pieces[3], DIAG)]
        si = sum(g.astype(F32) for g in got).astype(BF)
        gi = gather(si)
        *acts, _ = chain(chip, h0o, y0o, w1b, w2b, scale, acts)
        gl = []
        for l in range(nl):
            sp, sm = dw_half(core, acts, l)
            gl.append(gather((sm + send(sp, D2D)).astype(BF)))
        wi_n, mi_n, vi_n, wib = lamb(me, wi, mi, vi, gi, None, None, (), False, 384)
        b1, b2 = (), ()
        w1n, w2n = [], []
        for l in range(nl):
            *b1, wb = lamb(me, w1, m1, v1, gl[l], 1, l, b1, True, 384)
            w1n.append(wb)
            *b2, wb = lamb(me, w2, m2, v2, gl[l], 0, l, b2, False, 384)
            w2n.append(wb)
        h1 = forward(in_matmul(x1, wib), w1n, w2n)
        loss = jnp.sum((h1 - y1.astype(F32)) ** 2, axis=-1) / (2.0 * d)
        return (wi_n, b1[0], b2[0], mi_n, vi_n, b1[1], b1[2], b2[1], b2[2], loss, h1)

    w2s = P('rep', None)
    w3s = P('rep', None, None)
    ts = P(('rep', 'data'), None)
    return jax.shard_map(step, mesh=mesh,
                         in_specs=(w2s, w3s, w3s, w2s, w2s, w3s, w3s, w3s, w3s, ts, ts, ts, ts),
                         out_specs=(w2s, w3s, w3s, w2s, w2s, w3s, w3s, w3s, w3s, P(('rep', 'data')), ts),
                         check_vma=False)
```

```python
import functools

import jax
import jax.numpy as jnp
from jax import lax
from jax.experimental import pallas as pl
from jax.experimental.pallas import tpu as pltpu
from jax.sharding import PartitionSpec as P


BETA1 = 0.9
BETA2 = 0.999
BC1 = 1.0 / (1.0 - BETA1 ** 10)
BC2 = 1.0 / (1.0 - BETA2 ** 10)
EPS = 1e-12
WD = 0.01
ETA = 0.05
R2 = 0.7071067811865476
R2PI = 0.3989422804014327
BF = jnp.bfloat16
F32 = jnp.float32
VMEM = 67043328
ANY = pl.BlockSpec(memory_space=pl.ANY)

D2D = [(0, 1), (1, 0), (2, 3), (3, 2)]
CROSS = [(0, 2), (2, 0), (1, 3), (3, 1)]
DIAG = [(0, 3), (3, 0), (1, 2), (2, 1)]


def dot(a, b):
    return jnp.dot(a, b, preferred_element_type=F32)


def dot_nt(a, b):
    return lax.dot_general(a, b, (((1,), (1,)), ((), ())), preferred_element_type=F32)


def gelu(a):
    return (0.5 * a) * (1.0 + lax.erf(a * R2))


def gelu_grad(a):
    return 0.5 * (1.0 + lax.erf(a * R2)) + a * jnp.exp(-0.5 * a * a) * R2PI


def params(*sem):
    return pltpu.CompilerParams(vmem_limit_bytes=VMEM, dimension_semantics=sem)


def cost(flops, nbytes):
    return pl.CostEstimate(flops=int(flops), bytes_accessed=int(nbytes), transcendentals=0)


def in_kernel(x_ref, w_ref, o_ref):
    @pl.when(pl.program_id(0) == 0)
    def _():
        o_ref[...] = jnp.zeros_like(o_ref)

    o_ref[...] += dot(x_ref[...], w_ref[...].astype(BF))


def in_matmul(x, w, kb=768):
    t, e = x.shape
    d = w.shape[1]
    return pl.pallas_call(
        in_kernel,
        grid=(e // kb,),
        in_specs=[pl.BlockSpec((t, kb), lambda k: (0, k)), pl.BlockSpec((kb, d), lambda k: (k, 0))],
        out_specs=pl.BlockSpec((t, d), lambda k: (0, 0)),
        out_shape=jax.ShapeDtypeStruct((t, d), F32),
        compiler_params=params("arbitrary"),
        cost_estimate=cost(2 * t * e * d, 2 * t * e + w.nbytes + 4 * t * d),
    )(x, w)


def chain_kernel(scale, dev, nm, c_ref, h_ref, y_ref, w1_hbm, w2_hbm, *rest):
    t_o, p_o, g0_o, w1, w2, a_s, s_s, h_s, b_s, sem = rest[2 * (dev > 0):]
    t = pl.program_id(0)
    c = c_ref[0]
    nl, _, f = w1.shape
    half = f // 2
    fc = half // nm

    def copies(l):
        out = []
        for k in range(2):
            src = pl.multiple_of(lax.rem(c + k, 2) * half, half)
            out.append(pltpu.make_async_copy(w1_hbm.at[l, :, pl.ds(src, half)], w1.at[l, :, pl.ds(k * half, half)],
                                             sem.at[l, k]))
            out.append(pltpu.make_async_copy(w2_hbm.at[l, pl.ds(src, half), :], w2.at[l, pl.ds(k * half, half), :],
                                             sem.at[l, k + 2]))
        return out

    @pl.when(t == 0)
    def _():
        for l in range(nl):
            for cp in copies(l):
                cp.start()

    h_s[...] = h_ref[...]

    def piece(l, kind, j):
        return p_o.at[0, l, kind, :, j * fc:(j + 1) * fc] if j < nm else s_s.at[:, (j - nm) * fc:(j - nm + 1) * fc]

    def fwd(l, carry):
        @pl.when(t == 0)
        def _():
            for cp in copies(l):
                cp.wait()

        b_s[...] = h_s[...].astype(BF)

        def up(j):
            a_s[l, :, j * fc:(j + 1) * fc] = dot(b_s[...], w1[l, :, j * fc:(j + 1) * fc])

        up(0)
        t_o[0, l, 1] = b_s[...].T
        for j in range(2 * nm):
            if j + 1 < 2 * nm:
                up(j + 1)
            piece(l, 0, j)[...] = gelu(a_s[l, :, j * fc:(j + 1) * fc]).astype(BF)
            h_s[...] += dot(piece(l, 0, j)[...], w2[l, j * fc:(j + 1) * fc, :])
        return carry

    def bwd(k, carry):
        l = nl - 1 - k
        b_s[...] = h_s[...].astype(BF)

        def down(j):
            return dot_nt(b_s[...], w2[l, j * fc:(j + 1) * fc, :])

        de = down(0)
        t_o[0, l, 0] = b_s[...].T
        for j in range(2 * nm):
            nxt = down(j + 1) if j + 1 < 2 * nm else None
            piece(l, 1, j)[...] = (de * gelu_grad(a_s[l, :, j * fc:(j + 1) * fc])).astype(BF)
            h_s[...] += dot_nt(piece(l, 1, j)[...], w1[l, :, j * fc:(j + 1) * fc])
            de = nxt
        return carry

    lax.fori_loop(0, nl, fwd, 0)
    h_s[...] = (h_s[...] - y_ref[...].astype(F32)) * scale
    lax.fori_loop(0, nl, bwd, 0)
    g0_o[...] = h_s[...].astype(BF).T


def chain(c, h, y, w1, w2, scale, prev=None, tm=256, nm=2):
    t, d = h.shape
    nl, _, f = w1.shape
    half = f // 2
    dev = 0 if prev is None else 1
    tok = pl.BlockSpec((tm, d), lambda i, c: (i, 0))
    return pl.pallas_call(
        functools.partial(chain_kernel, scale, dev, nm),
        grid_spec=pltpu.PrefetchScalarGridSpec(
            num_scalar_prefetch=1,
            grid=(t // tm,),
            in_specs=[tok, tok, ANY, ANY] + [ANY] * (2 * dev),
            out_specs=[pl.BlockSpec((1, nl, 2, d, tm), lambda i, c: (dev, 0, 0, 0, i)),
                       pl.BlockSpec((1, nl, 2, tm, half), lambda i, c: (dev, 0, 0, i, 0)),
                       pl.BlockSpec((d, tm), lambda i, c: (0, i))],
            scratch_shapes=[
                pltpu.VMEM((nl, d, f), BF),
                pltpu.VMEM((nl, f, d), BF),
                pltpu.VMEM((nl, tm, f), F32),
                pltpu.VMEM((tm, half), BF),
                pltpu.VMEM((tm, d), F32),
                pltpu.VMEM((tm, d), BF),
                pltpu.SemaphoreType.DMA((nl, 4)),
            ],
        ),
        out_shape=[jax.ShapeDtypeStruct((2, nl, 2, d, t), BF), jax.ShapeDtypeStruct((2, nl, 2, t, half), BF),
                   jax.ShapeDtypeStruct((d, t), BF)],
        input_output_aliases={5 + k: k for k in range(2 * dev)},
        compiler_params=params("arbitrary"),
        cost_estimate=cost(8 * nl * t * d * f, 4 * nl * d * f + 8 * t * d + 4 * nl * t * (d + half)),
    )(c, h, y, w1, w2, *(prev or ()))


def dw_kernel(i_ref, t_ref, p_ref, o_ref):
    r = dot(t_ref[0, 0, 0], p_ref[0, 0, 0]).astype(BF).astype(F32)
    o_ref[0] = jnp.where(pl.program_id(1) == 0, 0.0, o_ref[0]) + r


def dw_half(core, acts, l):
    ts, ps = acts
    d, t = ts.shape[3:]
    q = ps.shape[4] // 2
    return pl.pallas_call(
        dw_kernel,
        grid_spec=pltpu.PrefetchScalarGridSpec(
            num_scalar_prefetch=1,
            grid=(4, 2),
            in_specs=[pl.BlockSpec((1, 1, 1, d, t), lambda job, dev, c: (dev, l, job % 2, 0, 0)),
                      pl.BlockSpec((1, 1, 1, t, q), lambda job, dev, c: (
                          dev, l, job % 2, 0, jnp.where(job < 2, 1 - c[0], c[0])))],
            out_specs=pl.BlockSpec((1, d, q), lambda job, dev, c: (job, 0, 0)),
        ),
        out_shape=jax.ShapeDtypeStruct((4, d, q), F32),
        compiler_params=params("arbitrary", "arbitrary"),
        cost_estimate=cost(16 * t * d * q, 16 * t * (d + q) + 16 * d * q),
    )(core, ts, ps)


def dwi_kernel(i_ref, g_ref, x_ref, *refs):
    acc = refs[-1]
    acc[...] = dot(g_ref[...], x_ref[...])
    for k in range(4):
        @pl.when(pl.program_id(0) == k)
        def _(k=k):
            refs[k][...] = acc[...].astype(BF)


def dwi_quarters(i, g, x, eb=512):
    t, e = x.shape
    d = g.shape[0]
    n = e // 4 // eb

    def quarter(k, i):
        return jnp.bitwise_xor(jnp.where(k == 0, 2, jnp.where(k == 1, 3, jnp.where(k == 2, 1, 0))), i[0])

    def at(kk):
        return lambda k, j, i: (0, jnp.where(k < kk, 0, jnp.where(k > kk, n - 1, j)))

    return pl.pallas_call(
        dwi_kernel,
        grid_spec=pltpu.PrefetchScalarGridSpec(
            num_scalar_prefetch=1,
            grid=(4, n),
            in_specs=[pl.BlockSpec((d, t), lambda k, j, i: (0, 0)),
                      pl.BlockSpec((t, eb), lambda k, j, i: (0, quarter(k, i) * n + j))],
            out_specs=[pl.BlockSpec((d, eb), at(kk)) for kk in range(4)],
            scratch_shapes=[pltpu.VMEM((d, eb), F32)],
        ),
        out_shape=[jax.ShapeDtypeStruct((d, e // 4), BF)] * 4,
        compiler_params=params("arbitrary", "arbitrary"),
        cost_estimate=cost(2 * t * e * d, 2 * t * (e + d) + 2 * d * e),
        name="dwi",
    )(i, g, x)


def lamb_kernel(nb, flip, i_ref, *refs):
    w_ref, m_ref, v_ref, g0, g1, g2, g3 = refs[:7]
    wn_o, mn_o, vn_o, wb_o, w_s, u_s, sw, su, ratio = refs[-9:]
    p, k, j = pl.program_id(0), pl.program_id(1), pl.program_id(2)
    slot = k * nb + j
    shape = w_s.shape[1:]
    first = (k == 0) & (j == 0)

    @pl.when((p == 0) & first)
    def _():
        sw[...] = jnp.zeros_like(sw)
        su[...] = jnp.zeros_like(su)

    def sweep(g_ref):
        w = w_ref[...].reshape(shape)
        g = g_ref[...].reshape(g_ref.shape[-2:]).astype(F32)
        g = g.T if flip else g
        m2 = BETA1 * m_ref[...].reshape(shape) + (1.0 - BETA1) * g
        v2 = BETA2 * v_ref[...].reshape(shape) + (1.0 - BETA2) * g * g
        u = BC1 * m2 / (jnp.sqrt(BC2 * v2) + EPS) + WD * w
        mn_o[...] = m2.reshape(mn_o.shape)
        vn_o[...] = v2.reshape(vn_o.shape)
        w_s[slot] = w
        u_s[slot] = u
        sw[...] += jnp.sum((w * w).reshape(-1, 8, shape[1]), axis=0)
        su[...] += jnp.sum((u * u).reshape(-1, 8, shape[1]), axis=0)

    for kk, g_ref in enumerate((g0, g1, g2, g3)):
        @pl.when((p == 0) & (k == kk))
        def _(g_ref=g_ref):
            sweep(g_ref)

    @pl.when((p == 1) & first)
    def _():
        ratio[0] = ETA * (jnp.sqrt(jnp.sum(sw[...])) / jnp.sqrt(jnp.sum(su[...])))

    @pl.when(p == 1)
    def _():
        w = w_s[slot] - ratio[0] * u_s[slot]
        wn_o[...] = w.reshape(wn_o.shape)
        wb_o[...] = w.astype(BF)


def lamb(i, w, m, v, gs, gi, l, bufs, cols, rb):
    rows, width = w.shape[-2:]
    gr, gw = gs[0].shape[-2:] if cols else gs[0].shape[:-3:-1]
    nb = gr // rb
    lead = () if l is None else (l,)
    one = () if l is None else (1,)

    def where(k, j, i):
        q = jnp.bitwise_xor(k, i[0])
        return (j, q) if cols else (q * nb + j, 0)

    def at_first(p, k, j, i):
        k, j = jnp.where(p == 0, k, 3), jnp.where(p == 0, j, nb - 1)
        return lead + where(k, j, i)

    def at_second(p, k, j, i):
        k, j = jnp.where(p == 1, k, 0), jnp.where(p == 1, j, 0)
        return lead + where(k, j, i)

    def at_second2(p, k, j, i):
        k, j = jnp.where(p == 1, k, 0), jnp.where(p == 1, j, 0)
        return where(k, j, i)

    def at_g(kk):
        def index(p, k, j, i):
            b = jnp.where((p == 1) | (k > kk), nb - 1, jnp.where(k < kk, 0, j))
            b = (b, 0) if cols else (0, b)
            return b if gi is None else (gi,) + b

        return index

    blk = one + (rb, gw)
    gblk = (rb, gw) if cols else (gw, rb)
    gblk = gblk if gi is None else (1,) + gblk
    n = len(bufs)
    f32 = jax.ShapeDtypeStruct(w.shape, F32)
    return pl.pallas_call(
        functools.partial(lamb_kernel, nb, not cols),
        grid_spec=pltpu.PrefetchScalarGridSpec(
            num_scalar_prefetch=1,
            grid=(2, 4, nb),
            in_specs=[pl.BlockSpec(blk, at_first)] * 3 + [pl.BlockSpec(gblk, at_g(kk)) for kk in range(4)] + [ANY] * n,
            out_specs=[pl.BlockSpec(blk, at_second), pl.BlockSpec(blk, at_first), pl.BlockSpec(blk, at_first),
                       pl.BlockSpec((rb, gw), at_second2)],
            scratch_shapes=[
                pltpu.VMEM((4 * nb, rb, gw), F32),
                pltpu.VMEM((4 * nb, rb, gw), F32),
                pltpu.VMEM((8, gw), F32),
                pltpu.VMEM((8, gw), F32),
                pltpu.SMEM((1,), F32),
            ],
        ),
        out_shape=[f32, f32, f32, jax.ShapeDtypeStruct((rows, width), BF)],
        input_output_aliases={8 + k: k for k in range(n)},
        compiler_params=params("arbitrary", "arbitrary", "arbitrary"),
        cost_estimate=cost(30 * rows * width * 30, 28 * rows * width),
    )(i, w, m, v, *gs, *bufs)


def fwd_kernel(nl, nj, h_ref, *refs):
    w1_hbm, w2_hbm = refs[:nl], refs[nl:2 * nl]
    o_ref, w1, w2, a_s, s_s, sem = refs[2 * nl:]
    t = pl.program_id(0)
    fc = w1.shape[2] // nj

    @pl.when(t == 0)
    def _():
        for l in range(nl):
            pltpu.make_async_copy(w1_hbm[l], w1.at[l], sem.at[l, 0]).start()
            pltpu.make_async_copy(w2_hbm[l], w2.at[l], sem.at[l, 1]).start()

    o_ref[...] = h_ref[...]

    def layer(l, carry):
        @pl.when(t == 0)
        def _():
            pltpu.make_async_copy(w1_hbm[0], w1.at[l], sem.at[l, 0]).wait()
            pltpu.make_async_copy(w2_hbm[0], w2.at[l], sem.at[l, 1]).wait()

        hb = o_ref[...].astype(BF)

        def up(j):
            a_s[:, j * fc:(j + 1) * fc] = dot(hb, w1[l, :, j * fc:(j + 1) * fc])

        up(0)
        for j in range(nj):
            if j + 1 < nj:
                up(j + 1)
            s_s[:, j * fc:(j + 1) * fc] = gelu(a_s[:, j * fc:(j + 1) * fc]).astype(BF)
            o_ref[...] += dot(s_s[:, j * fc:(j + 1) * fc], w2[l, j * fc:(j + 1) * fc, :])
        return carry

    lax.fori_loop(0, nl, layer, 0)


def forward(h, w1, w2, tm=256, nj=4):
    t, d = h.shape
    nl = len(w1)
    f = w1[0].shape[1]
    tok = pl.BlockSpec((tm, d), lambda i: (i, 0))
    return pl.pallas_call(
        functools.partial(fwd_kernel, nl, nj),
        grid=(t // tm,),
        in_specs=[tok] + [ANY] * (2 * nl),
        out_specs=tok,
        out_shape=jax.ShapeDtypeStruct((t, d), F32),
        scratch_shapes=[
            pltpu.VMEM((nl, d, f), BF),
            pltpu.VMEM((nl, f, d), BF),
            pltpu.VMEM((tm, f), F32),
            pltpu.VMEM((tm, f), BF),
            pltpu.SemaphoreType.DMA((nl, 2)),
        ],
        compiler_params=params("arbitrary"),
        cost_estimate=cost(4 * nl * t * d * f, 4 * nl * d * f + 8 * t * d),
        name="forward",
    )(h, *w1, *w2)


def solution(mesh):
    p = mesh.shape['data']

    def inner(wi, w1, w2, mi, vi, m1, v1, m2, v2, x0, y0, x1, y1):
        nl, d, _ = w1.shape
        scale = 1.0 / (x0.shape[0] * p * d)
        i = lax.axis_index('data').astype(jnp.int32)
        me = jnp.reshape(i, (1,))
        chip = me // 2
        core = me % 2

        def send(x, perm):
            return lax.ppermute(x, 'data', perm)

        def gather(g):
            far = send(g, CROSS)
            return g, send(g, D2D), far, send(far, D2D)

        y0o = send(y0, CROSS)
        h0 = in_matmul(x0, wi)
        h0o = send(h0, CROSS)
        w1b, w2b = w1.astype(BF), w2.astype(BF)
        *acts, g0 = chain(chip, h0, y0, w1b, w2b, scale)
        *far, near, own = dwi_quarters(me, g0, x0)
        got = [own, send(near, D2D), send(far[0], CROSS), send(far[1], DIAG)]
        *acts, _ = chain(chip, h0o, y0o, w1b, w2b, scale, lax.optimization_barrier((acts, own))[0])
        got, acts = lax.optimization_barrier((got, acts))
        si = sum(g.astype(F32) for g in got).astype(BF)
        gi = gather(si)
        gl = []
        for l in range(nl):
            acts = lax.optimization_barrier((acts, si if l == 0 else parts if l == 1 else gl[-1][0]))[0]
            last = parts if l else None
            parts = dw_half(core, acts, l)
            if l:
                gl.append(gather((last[2:] + other[:2]).astype(BF)))
            other = send(parts, D2D)
        gl.append(gather((parts[2:] + other[:2]).astype(BF)))
        wi_n, mi_n, vi_n, wib = lamb(me, wi, mi, vi, gi, None, None, (), False, 384)
        b1, b2 = (), ()
        w1n, w2n = [], []
        for l in range(nl):
            *b1, wb = lamb(me, w1, m1, v1, gl[l], 1, l, b1, True, 384)
            w1n.append(wb)
            *b2, wb = lamb(me, w2, m2, v2, gl[l], 0, l, b2, False, 384)
            w2n.append(wb)
        h1 = forward(in_matmul(x1, wib), w1n, w2n)
        loss = jnp.sum((h1 - y1.astype(F32)) ** 2, axis=-1) / (2.0 * d)
        return (wi_n, b1[0], b2[0], mi_n, vi_n, b1[1], b1[2], b2[1], b2[2], loss, h1)

    w2s = P('rep', None)
    w3s = P('rep', None, None)
    ts = P(('rep', 'data'), None)
    return jax.shard_map(inner, mesh=mesh,
                         in_specs=(w2s, w3s, w3s, w2s, w2s, w3s, w3s, w3s, w3s, ts, ts, ts, ts),
                         out_specs=(w2s, w3s, w3s, w2s, w2s, w3s, w3s, w3s, w3s, P(('rep', 'data')), ts),
                         check_vma=False)
```

```python
import functools

import jax
import jax.numpy as jnp
from jax import lax
from jax.experimental import pallas as pl
from jax.experimental.pallas import tpu as pltpu
from jax.sharding import PartitionSpec as P


BETA1 = 0.9
BETA2 = 0.999
BC1 = 1.0 / (1.0 - BETA1 ** 10)
BC2 = 1.0 / (1.0 - BETA2 ** 10)
EPS = 1e-12
WD = 0.01
ETA = 0.05
R2 = 0.7071067811865476
R2PI = 0.3989422804014327
BF = jnp.bfloat16
F32 = jnp.float32
VMEM = 67043328
ANY = pl.BlockSpec(memory_space=pl.ANY)

D2D = [(0, 1), (1, 0), (2, 3), (3, 2)]
CROSS = [(0, 2), (2, 0), (1, 3), (3, 1)]
DIAG = [(0, 3), (3, 0), (1, 2), (2, 1)]


def dot(a, b):
    return jnp.dot(a, b, preferred_element_type=F32)


def dot_nt(a, b):
    return lax.dot_general(a, b, (((1,), (1,)), ((), ())), preferred_element_type=F32)


def gelu(a):
    return (0.5 * a) * (1.0 + lax.erf(a * R2))


def gelu_grad(a):
    return 0.5 * (1.0 + lax.erf(a * R2)) + a * jnp.exp(-0.5 * a * a) * R2PI


def params(*sem):
    return pltpu.CompilerParams(vmem_limit_bytes=VMEM, dimension_semantics=sem)


def cost(flops, nbytes):
    return pl.CostEstimate(flops=int(flops), bytes_accessed=int(nbytes), transcendentals=0)


def in_kernel(x_ref, w_ref, o_ref):
    @pl.when(pl.program_id(0) == 0)
    def _():
        o_ref[...] = jnp.zeros_like(o_ref)

    o_ref[...] += dot(x_ref[...], w_ref[...].astype(BF))


def in_matmul(x, w, kb=768):
    t, e = x.shape
    d = w.shape[1]
    return pl.pallas_call(
        in_kernel,
        grid=(e // kb,),
        in_specs=[pl.BlockSpec((t, kb), lambda k: (0, k)), pl.BlockSpec((kb, d), lambda k: (k, 0))],
        out_specs=pl.BlockSpec((t, d), lambda k: (0, 0)),
        out_shape=jax.ShapeDtypeStruct((t, d), F32),
        compiler_params=params("arbitrary"),
        cost_estimate=cost(2 * t * e * d, 2 * t * e + w.nbytes + 4 * t * d),
    )(x, w)


def chain_kernel(scale, dev, nm, c_ref, h_ref, y_ref, w1_hbm, w2_hbm, *rest):
    t_o, p_o, g0_o, w1, w2, a_s, s_s, h_s, b_s, sem = rest[2 * (dev > 0):]
    t = pl.program_id(0)
    c = c_ref[0]
    nl, _, f = w1.shape
    half = f // 2
    fc = half // nm

    def copies(l):
        out = []
        for k in range(2):
            src = pl.multiple_of(lax.rem(c + k, 2) * half, half)
            out.append(pltpu.make_async_copy(w1_hbm.at[l, :, pl.ds(src, half)], w1.at[l, :, pl.ds(k * half, half)],
                                             sem.at[l, k]))
            out.append(pltpu.make_async_copy(w2_hbm.at[l, pl.ds(src, half), :], w2.at[l, pl.ds(k * half, half), :],
                                             sem.at[l, k + 2]))
        return out

    @pl.when(t == 0)
    def _():
        for l in range(nl):
            for cp in copies(l):
                cp.start()

    h_s[...] = h_ref[...]

    def fwd(l, carry):
        @pl.when(t == 0)
        def _():
            for cp in copies(l):
                cp.wait()

        b_s[...] = h_s[...].astype(BF)

        def up(j):
            a_s[l, :, j * fc:(j + 1) * fc] = dot(b_s[...], w1[l, :, j * fc:(j + 1) * fc])

        up(0)
        t_o[0, l, nm] = b_s[...].T
        for j in range(2 * nm):
            if j + 1 < 2 * nm:
                up(j + 1)
            s_s[:, j * fc:(j + 1) * fc] = gelu(a_s[l, :, j * fc:(j + 1) * fc]).astype(BF)
            h_s[...] += dot(s_s[:, j * fc:(j + 1) * fc], w2[l, j * fc:(j + 1) * fc, :])
            if j < nm:
                t_o[0, l, j] = s_s[:, j * fc:(j + 1) * fc].T
        return carry

    def bwd(k, carry):
        l = nl - 1 - k
        p_o[0, l, 0] = h_s[...].astype(BF)

        def down(j):
            return dot_nt(p_o[0, l, 0], w2[l, j * fc:(j + 1) * fc, :])

        def piece(j):
            return p_o.at[0, l, 1 + j] if j < nm else s_s.at[:, j * fc:(j + 1) * fc]

        de = down(0)
        for j in range(2 * nm):
            nxt = down(j + 1) if j + 1 < 2 * nm else None
            piece(j)[...] = (de * gelu_grad(a_s[l, :, j * fc:(j + 1) * fc])).astype(BF)
            h_s[...] += dot_nt(piece(j)[...], w1[l, :, j * fc:(j + 1) * fc])
            de = nxt
        return carry

    lax.fori_loop(0, nl, fwd, 0)
    h_s[...] = (h_s[...] - y_ref[...].astype(F32)) * scale
    lax.fori_loop(0, nl, bwd, 0)
    g0_o[...] = h_s[...].astype(BF).T


def chain(c, h, y, w1, w2, scale, prev=None, tm=256, nm=2):
    t, d = h.shape
    nl, _, f = w1.shape
    dev = 0 if prev is None else 1
    tok = pl.BlockSpec((tm, d), lambda i, c: (i, 0))
    return pl.pallas_call(
        functools.partial(chain_kernel, scale, dev, nm),
        grid_spec=pltpu.PrefetchScalarGridSpec(
            num_scalar_prefetch=1,
            grid=(t // tm,),
            in_specs=[tok, tok, ANY, ANY] + [ANY] * (2 * dev),
            out_specs=[pl.BlockSpec((1, nl, nm + 1, d, tm), lambda i, c: (dev, 0, 0, 0, i)),
                       pl.BlockSpec((1, nl, nm + 1, tm, d), lambda i, c: (dev, 0, 0, i, 0)),
                       pl.BlockSpec((d, tm), lambda i, c: (0, i))],
            scratch_shapes=[
                pltpu.VMEM((nl, d, f), BF),
                pltpu.VMEM((nl, f, d), BF),
                pltpu.VMEM((nl, tm, f), F32),
                pltpu.VMEM((tm, f), BF),
                pltpu.VMEM((tm, d), F32),
                pltpu.VMEM((tm, d), BF),
                pltpu.SemaphoreType.DMA((nl, 4)),
            ],
        ),
        out_shape=[jax.ShapeDtypeStruct((2, nl, nm + 1, d, t), BF), jax.ShapeDtypeStruct((2, nl, nm + 1, t, d), BF),
                   jax.ShapeDtypeStruct((d, t), BF)],
        input_output_aliases={5 + k: k for k in range(2 * dev)},
        compiler_params=params("arbitrary"),
        cost_estimate=cost(8 * nl * t * d * f, 4 * nl * d * f + 8 * t * d + 4 * nl * t * 3 * d),
    )(c, h, y, w1, w2, *(prev or ()))


def dw_kernel(i_ref, t_ref, p_ref, o_ref):
    r = dot(t_ref[0, 0, 0], p_ref[0, 0, 0]).astype(BF).astype(F32)
    o_ref[0] = jnp.where(pl.program_id(1) == 0, 0.0, o_ref[0]) + r


def dw_half(core, acts, l):
    ts, ps = acts
    d, t = ts.shape[3:]

    def quarter(job, c):
        return jnp.where(job < 2, 1 - c[0], c[0])

    def tplane(job, dev, c):
        return (dev, l, jnp.where(job % 2 == 0, quarter(job, c), 2), 0, 0)

    def pplane(job, dev, c):
        return (dev, l, jnp.where(job % 2 == 0, 0, quarter(job, c) + 1), 0, 0)

    return pl.pallas_call(
        dw_kernel,
        grid_spec=pltpu.PrefetchScalarGridSpec(
            num_scalar_prefetch=1,
            grid=(4, 2),
            in_specs=[pl.BlockSpec((1, 1, 1, d, t), tplane), pl.BlockSpec((1, 1, 1, t, d), pplane)],
            out_specs=pl.BlockSpec((1, d, d), lambda job, dev, c: (job, 0, 0)),
        ),
        out_shape=jax.ShapeDtypeStruct((4, d, d), F32),
        compiler_params=params("arbitrary", "arbitrary"),
        cost_estimate=cost(16 * t * d * d, 32 * t * d + 16 * d * d),
    )(core, ts, ps)


def dwi_kernel(i_ref, g_ref, x_ref, *refs):
    acc = refs[-1]
    acc[...] = dot(g_ref[...], x_ref[...]).T
    for k in range(4):
        @pl.when(pl.program_id(0) == k)
        def _(k=k):
            refs[k][...] = acc[...].astype(BF)


def dwi_quarters(i, g, x, eb=512):
    t, e = x.shape
    d = g.shape[0]
    n = e // 4 // eb

    def quarter(k, i):
        return jnp.bitwise_xor(jnp.where(k == 0, 2, jnp.where(k == 1, 3, jnp.where(k == 2, 1, 0))), i[0])

    def at(kk):
        return lambda k, j, i: (jnp.where(k < kk, 0, jnp.where(k > kk, n - 1, j)), 0)

    return pl.pallas_call(
        dwi_kernel,
        grid_spec=pltpu.PrefetchScalarGridSpec(
            num_scalar_prefetch=1,
            grid=(4, n),
            in_specs=[pl.BlockSpec((d, t), lambda k, j, i: (0, 0)),
                      pl.BlockSpec((t, eb), lambda k, j, i: (0, quarter(k, i) * n + j))],
            out_specs=[pl.BlockSpec((eb, d), at(kk)) for kk in range(4)],
            scratch_shapes=[pltpu.VMEM((eb, d), F32)],
        ),
        out_shape=[jax.ShapeDtypeStruct((e // 4, d), BF)] * 4,
        compiler_params=params("arbitrary", "arbitrary"),
        cost_estimate=cost(2 * t * e * d, 2 * t * (e + d) + 2 * d * e),
        name="dwi",
    )(i, g, x)


RB = 192
STRIP = 16
RING = 6
AHEAD = 3


class Forward:
    TM = 256

    def __init__(self, h, w1, w2):
        self.args = (h, w1, w2)
        self.t, self.d = h.shape
        self.nc, _, self.fc = w1.shape
        self.units = self.t // self.TM * self.nc
        self.flops = 4 * self.t * self.d * self.nc * self.fc
        nt = self.t // self.TM
        self.scratch = [
            pltpu.VMEM(w1.shape, BF),
            pltpu.VMEM(w2.shape, BF),
            pltpu.VMEM((nt, self.TM, self.d), F32),
            pltpu.VMEM((self.TM, self.d), BF),
            pltpu.VMEM((self.TM, self.fc), F32),
            pltpu.VMEM((self.TM, self.fc), BF),
            pltpu.SemaphoreType.DMA((self.nc,)),
            pltpu.SemaphoreType.DMA((nt,)),
        ]

    def bind(self, ins, out, scratch):
        self.h, self.w1, self.w2 = ins
        self.out = out
        self.w1_s, self.w2_s, self.h_s, self.b_s, self.a_s, self.s_s, self.wsem, self.hsem = scratch

    def tile(self, t):
        return pltpu.make_async_copy(self.h.at[pl.ds(pl.multiple_of(t * self.TM, self.TM), self.TM)], self.h_s.at[t],
                                     self.hsem.at[t])

    def weights(self, c):
        return (pltpu.make_async_copy(self.w1.at[c], self.w1_s.at[c], self.wsem.at[c]),
                pltpu.make_async_copy(self.w2.at[c], self.w2_s.at[c], self.wsem.at[c]))

    def start(self):
        for c in range(self.nc):
            if c < self.t // self.TM:
                self.tile(c).start()
            for cp in self.weights(c):
                cp.start()
        for t in range(self.nc, self.t // self.TM):
            self.tile(t).start()
        self.s_s[...] = jnp.zeros_like(self.s_s)

    def before(self, n):
        @pl.when(n < self.nc)
        def _():
            for cp in self.weights(n):
                cp.wait()

        @pl.when(n % self.nc == 0)
        def _():
            t = n // self.nc
            self.tile(t).wait()
            self.b_s[...] = self.h_s[t].astype(BF)

    def down(self, n, n0):
        t, c = n // self.nc, n % self.nc
        self.h_s[t, :, n0:n0 + 256] += dot(self.s_s[...], self.w2_s[c, :, n0:n0 + 256])

    def work(self, n):
        last = jnp.maximum(n - 1, 0)
        c = n % self.nc

        def up(n0):
            self.a_s[:, n0:n0 + 256] = dot(self.b_s[...], self.w1_s[c, :, n0:n0 + 256])

        return ([functools.partial(self.down, last, n0) for n0 in range(0, self.d, 256)]
                + [functools.partial(up, n0) for n0 in range(0, self.fc, 256)])

    def after(self, n):
        for r in range(0, self.TM, STRIP):
            self.s_s[r:r + STRIP] = gelu(self.a_s[r:r + STRIP]).astype(BF)

    def finish(self):
        for n0 in range(0, self.d, 256):
            self.down(self.units - 1, n0)
        nt = self.t // self.TM
        out = [pltpu.make_async_copy(self.h_s.at[t], self.out.at[pl.ds(t * self.TM, self.TM)], self.hsem.at[t])
               for t in range(nt)]
        for cp in out:
            cp.start()
        return out


class Input:
    KB = 768
    XR = 4

    def __init__(self, x, w):
        self.args = (x, w)
        self.t, self.e = x.shape
        self.d = w.shape[-1]
        self.mb = self.t // 4
        self.units = 4 * self.e // self.KB
        self.flops = 2 * self.t * self.e * self.d
        self.scratch = [
            pltpu.VMEM((self.XR, self.mb, self.KB), BF),
            pltpu.VMEM((2, self.KB, self.d), BF),
            pltpu.VMEM((4, self.mb, self.d), F32),
            pltpu.SemaphoreType.DMA((self.XR,)),
            pltpu.SemaphoreType.DMA((2,)),
            pltpu.SemaphoreType.DMA((1,)),
        ]

    def bind(self, ins, out, scratch):
        self.x, self.w = ins
        self.out = out
        self.x_s, self.w_s, self.h_s, self.xsem, self.wsem, self.osem = scratch

    def xcopy(self, n):
        src = self.x.at[pl.ds(pl.multiple_of(n % 4 * self.mb, self.mb), self.mb),
                        pl.ds(pl.multiple_of(n // 4 * self.KB, self.KB), self.KB)]
        return pltpu.make_async_copy(src, self.x_s.at[n % self.XR], self.xsem.at[n % self.XR])

    def wcopy(self, k):
        return pltpu.make_async_copy(self.w.at[k], self.w_s.at[k % 2], self.wsem.at[k % 2])

    def start(self):
        self.wcopy(0).start()
        for n in range(self.XR - 1):
            self.xcopy(n).start()
        self.h_s[...] = jnp.zeros_like(self.h_s)

    def before(self, n):
        self.xcopy(n).wait()

        @pl.when(n + self.XR - 1 < self.units)
        def _():
            self.xcopy(n + self.XR - 1).start()

        @pl.when(n % 4 == 0)
        def _():
            self.wcopy(n // 4).wait()

            @pl.when(n + 4 < self.units)
            def _():
                self.wcopy(n // 4 + 1).start()

    def work(self, n):
        m, xr, wr = n % 4, n % self.XR, n // 4 % 2

        def part(n0):
            self.h_s[m, :, n0:n0 + 256] += dot(self.x_s[xr], self.w_s[wr, :, n0:n0 + 256])

        return [functools.partial(part, n0) for n0 in range(0, self.d, 256)]

    def after(self, n):
        pass

    def finish(self):
        out = [pltpu.make_async_copy(self.h_s.at[m], self.out.at[pl.ds(m * self.mb, self.mb)], self.osem.at[0])
               for m in range(4)]
        for cp in out:
            cp.start()
        return out


def lamb_kernel(mats, job, *refs):
    i_ref, refs = refs[0], list(refs[1:])

    def take(n):
        out = refs[:n]
        del refs[:n]
        return out

    nm = len(mats)
    state = [take(3) for _ in mats]
    pieces = take(4)
    ins = take(len(job.args)) if job else []
    take(sum(3 for mat in mats if mat[3]))
    outs = [take(3) for _ in mats]
    lows = take(nm)
    out = take(1)[0] if job else None
    w_s, u_s, mv, g_s, b_s, sw, su, ratio, isem, osem, wsem, bsem = take(12)
    if job:
        job.bind(ins, out, refs)
    i = i_ref[0]
    nq = mats[0][2]
    nb = 4 * nq
    width = w_s.shape[2]
    qrows = nq * RB

    def block(m, ref, b):
        l = mats[m][0]
        q = jnp.bitwise_xor(b // nq, i)
        r = b % nq * RB
        if l is None:
            return ref.at[pl.ds(pl.multiple_of(q * qrows + r, RB), RB)]
        if ref.shape[2] == width:
            return ref.at[l, pl.ds(pl.multiple_of(q * qrows + r, RB), RB)]
        return ref.at[l, pl.ds(pl.multiple_of(r, RB), RB), pl.ds(pl.multiple_of(q * width, width), width)]

    def loads(m, b, n):
        r = n % RING
        w, mm, v = state[m]
        return (pltpu.make_async_copy(block(m, w, b), w_s.at[b], isem.at[r]),
                pltpu.make_async_copy(block(m, mm, b), mv.at[r, 0], isem.at[r]),
                pltpu.make_async_copy(block(m, v, b), mv.at[r, 1], isem.at[r]))

    def piece(m, k, b, n):
        gi = mats[m][1]
        src = pieces[k] if gi is None else pieces[k].at[gi]
        r = n % RING
        return pltpu.make_async_copy(src.at[pl.ds(pl.multiple_of(b % nq * RB, RB), RB)], g_s.at[r], isem.at[r])

    def load(m, b, n):
        for cp in loads(m, b, n):
            cp.start()
        for k in range(4):
            @pl.when(b // nq == k)
            def _(k=k):
                piece(m, k, b, n).start()

    def stores(m, b, n):
        r = n % RING
        return (pltpu.make_async_copy(mv.at[r, 0], block(m, outs[m][1], b), osem.at[r]),
                pltpu.make_async_copy(mv.at[r, 1], block(m, outs[m][2], b), osem.at[r]))

    def new(m, b):
        return pltpu.make_async_copy(w_s.at[b], block(m, outs[m][0], b), wsem.at[b])

    def low(m, b):
        q = jnp.bitwise_xor(b // nq, i)
        row = pl.multiple_of(q * qrows + b % nq * RB, RB)
        return pltpu.make_async_copy(b_s.at[b], lows[m].at[pl.ds(row, RB)], bsem.at[0])

    def strip(b, r, r0, sums):
        sl = pl.ds(r0, STRIP)
        w = w_s[b, sl]
        g = g_s[r, sl].astype(F32)
        m2 = BETA1 * mv[r, 0, sl] + (1.0 - BETA1) * g
        v2 = BETA2 * mv[r, 1, sl] + (1.0 - BETA2) * g * g
        u = BC1 * m2 / (jnp.sqrt(BC2 * v2) + EPS) + WD * w
        mv[r, 0, sl] = m2
        mv[r, 1, sl] = v2
        u_s[b, sl] = u
        for k in range(0, STRIP, 8):
            sums[0] = sums[0] + w[k:k + 8] * w[k:k + 8]
            sums[1] = sums[1] + u[k:k + 8] * u[k:k + 8]

    for b in range(AHEAD):
        load(0, b, b)
    if job:
        job.start()

    for m in range(nm):
        base = m * nb
        if m:
            for b in range(AHEAD):
                new(m - 1, b).wait()
                load(m, b, base + b)
        sw[...] = jnp.zeros_like(sw)
        su[...] = jnp.zeros_like(su)

        def sweep(b, carry):
            n = base + b
            r = n % RING
            for cp in loads(m, b, n):
                cp.wait()
            piece(m, 0, b, n).wait()

            @pl.when(n >= RING - AHEAD)
            def _():
                for cp in stores(m, b, n - (RING - AHEAD)):
                    cp.wait()

            @pl.when(b + AHEAD < nb)
            def _():
                if m:
                    new(m - 1, b + AHEAD).wait()
                load(m, b + AHEAD, n + AHEAD)

            sums = [jnp.zeros(sw.shape, F32), jnp.zeros(su.shape, F32)]
            if job:
                job.before(n)
            tasks = job.work(n) if job else []
            strips = list(range(0, RB, STRIP))
            per = -(-len(strips) // max(1, len(tasks)))
            for task in tasks:
                task()
                for r0 in strips[:per]:
                    strip(b, r, r0, sums)
                del strips[:per]
            for r0 in strips:
                strip(b, r, r0, sums)
            if job:
                job.after(n)
            sw[...] += sums[0]
            su[...] += sums[1]
            for cp in stores(m, b, n):
                cp.start()
            return carry

        lax.fori_loop(0, nb, sweep, 0)
        ratio[0] = ETA * (jnp.sqrt(jnp.sum(sw[...])) / jnp.sqrt(jnp.sum(su[...])))
        if job and m == nm - 1:
            flying = job.finish()

        def update(b, carry):
            if m:
                low(m - 1, b).wait()
            rt = ratio[0]
            for r0 in range(0, RB, STRIP):
                sl = pl.ds(r0, STRIP)
                w = w_s[b, sl] - rt * u_s[b, sl]
                w_s[b, sl] = w
                b_s[b, sl] = w.astype(BF)
            new(m, b).start()
            low(m, b).start()
            return carry

        lax.fori_loop(0, nb, update, 0)

    def drain(b, carry):
        new(nm - 1, b).wait()
        low(nm - 1, b).wait()
        return carry

    lax.fori_loop(0, nb, drain, 0)
    for n in range(nm * nb - (RING - AHEAD), nm * nb):
        for cp in stores(nm - 1, 0, n):
            cp.wait()
    if job:
        for cp in flying:
            cp.wait()


def lamb(i, mats, pieces, job=None):
    width = pieces[0].shape[-1]
    nq = pieces[0].shape[-2] // RB
    nb = 4 * nq
    args, outs, lows, bufs, aliases = [], [], [], [], {}
    for w, m, v, l, gi, old in mats:
        args += [w, m, v]
        outs += [jax.ShapeDtypeStruct(w.shape, F32)] * 3
        lows.append(jax.ShapeDtypeStruct((nb * RB, width), BF))
    args += pieces
    if job:
        args += job.args
    for k, mat in enumerate(mats):
        if mat[5] is not None:
            for c in range(3):
                aliases[1 + len(args) + len(bufs)] = 3 * k + c
                bufs.append(mat[5][c])
    size = nb * RB * width * len(mats)
    res = pl.pallas_call(
        functools.partial(lamb_kernel, [(l, gi, nq, old is not None) for _, _, _, l, gi, old in mats], job),
        in_specs=[pl.BlockSpec(memory_space=pltpu.SMEM)] + [ANY] * (len(args) + len(bufs)),
        out_specs=[ANY] * (len(outs) + len(lows) + bool(job)),
        out_shape=outs + lows + ([jax.ShapeDtypeStruct((job.t, job.d), F32)] if job else []),
        scratch_shapes=[
            pltpu.VMEM((nb, RB, width), F32),
            pltpu.VMEM((nb, RB, width), F32),
            pltpu.VMEM((RING, 2, RB, width), F32),
            pltpu.VMEM((RING, RB, width), BF),
            pltpu.VMEM((nb, RB, width), BF),
            pltpu.VMEM((8, width), F32),
            pltpu.VMEM((8, width), F32),
            pltpu.SMEM((1,), F32),
            pltpu.SemaphoreType.DMA((RING,)),
            pltpu.SemaphoreType.DMA((RING,)),
            pltpu.SemaphoreType.DMA((nb,)),
            pltpu.SemaphoreType.DMA((1,)),
        ] + (job.scratch if job else []),
        input_output_aliases=aliases,
        compiler_params=params(),
        cost_estimate=cost(1200 * size, 28 * size),
    )(i, *args, *bufs)
    n = len(mats)
    return [(res[3 * k:3 * k + 3], res[3 * n + k]) for k in range(n)], res[4 * n] if job else None


def last_kernel(h_ref, w1_hbm, w2_hbm, o_ref, w1, w2, a_s, s_s, b_s, sem):
    t = pl.program_id(0)
    nc = w1.shape[0]
    fc = w1.shape[2]

    def copies(c):
        return (pltpu.make_async_copy(w1_hbm.at[c], w1.at[c], sem.at[0, c]),
                pltpu.make_async_copy(w2_hbm.at[c], w2.at[c], sem.at[1, c]))

    @pl.when(t == 0)
    def _():
        for c in range(nc):
            for cp in copies(c):
                cp.start()
        for c in range(nc):
            for cp in copies(c):
                cp.wait()

    o_ref[...] = h_ref[...]
    b_s[...] = h_ref[...].astype(BF)

    def up(c):
        a_s[:, c * fc:(c + 1) * fc] = dot(b_s[...], w1[c])

    up(0)
    for c in range(nc):
        if c + 1 < nc:
            up(c + 1)
        s_s[:, c * fc:(c + 1) * fc] = gelu(a_s[:, c * fc:(c + 1) * fc]).astype(BF)
        o_ref[...] += dot(s_s[:, c * fc:(c + 1) * fc], w2[c])


def last_block(h, w1, w2, tm=256):
    t, d = h.shape
    nc, _, fc = w1.shape
    tok = pl.BlockSpec((tm, d), lambda i: (i, 0))
    return pl.pallas_call(
        last_kernel,
        grid=(t // tm,),
        in_specs=[tok, ANY, ANY],
        out_specs=tok,
        out_shape=jax.ShapeDtypeStruct((t, d), F32),
        scratch_shapes=[
            pltpu.VMEM(w1.shape, BF),
            pltpu.VMEM(w2.shape, BF),
            pltpu.VMEM((tm, nc * fc), F32),
            pltpu.VMEM((tm, nc * fc), BF),
            pltpu.VMEM((tm, d), BF),
            pltpu.SemaphoreType.DMA((2, nc)),
        ],
        compiler_params=params("arbitrary"),
        cost_estimate=cost(4 * t * d * nc * fc, 4 * d * nc * fc + 8 * t * d),
        name="last",
    )(h, w1, w2)


def solution(mesh):
    p = mesh.shape['data']

    def inner(wi, w1, w2, mi, vi, m1, v1, m2, v2, x0, y0, x1, y1):
        nl, d, _ = w1.shape
        scale = 1.0 / (x0.shape[0] * p * d)
        i = lax.axis_index('data').astype(jnp.int32)
        me = jnp.reshape(i, (1,))
        chip = me // 2
        core = me % 2

        def send(x, perm):
            return lax.ppermute(x, 'data', perm)

        def gather(g):
            far = send(g, CROSS)
            return g, send(g, D2D), far, send(far, D2D)

        y0o = send(y0, CROSS)
        h0 = in_matmul(x0, wi)
        h0o = send(h0, CROSS)
        w1b, w2b = w1.astype(BF), w2.astype(BF)
        *acts, g0 = chain(chip, h0, y0, w1b, w2b, scale)
        *far, near, own = dwi_quarters(me, g0, x0)
        got = [own, send(near, D2D), send(far[0], CROSS), send(far[1], DIAG)]
        *acts, _ = chain(chip, h0o, y0o, w1b, w2b, scale, lax.optimization_barrier((acts, own))[0])
        got, acts = lax.optimization_barrier((got, acts))
        si = sum(g.astype(F32) for g in got).astype(BF)
        gi = gather(si)
        gl = []
        for l in range(nl):
            acts = lax.optimization_barrier((acts, si if l == 0 else parts if l == 1 else gl[-1][0]))[0]
            last = parts if l else None
            parts = dw_half(core, acts, l)
            if l:
                gl.append(gather((last[2:] + other[:2]).astype(BF)))
            other = send(parts, D2D)
        gl.append(gather((parts[2:] + other[:2]).astype(BF)))
        [((wi_n, mi_n, vi_n), wib)], _ = lamb(me, [(wi, mi, vi, None, None, None)], gi)
        b1 = b2 = None
        h1 = None
        for l in range(nl):
            job = Input(x1, wib.reshape(-1, d, d)) if l == 0 else Forward(h1, wb1, wb2)
            [(b1, wb1), (b2, wb2)], h1 = lamb(me, [(w1, m1, v1, l, 1, b1), (w2, m2, v2, l, 0, b2)], gl[l], job)
            wb1, wb2 = wb1.reshape(-1, d, d), wb2.reshape(-1, d, d)
        h1 = last_block(h1, wb1, wb2)
        loss = jnp.sum((h1 - y1.astype(F32)) ** 2, axis=-1) / (2.0 * d)
        return (wi_n, b1[0], b2[0], mi_n, vi_n, b1[1], b1[2], b2[1], b2[2], loss, h1)

    w2s = P('rep', None)
    w3s = P('rep', None, None)
    ts = P(('rep', 'data'), None)
    return jax.shard_map(inner, mesh=mesh,
                         in_specs=(w2s, w3s, w3s, w2s, w2s, w3s, w3s, w3s, w3s, ts, ts, ts, ts),
                         out_specs=(w2s, w3s, w3s, w2s, w2s, w3s, w3s, w3s, w3s, P(('rep', 'data')), ts),
                         check_vma=False)
```
